128 devices in a mesh: leaf: 128 (over x, z, y, core).
Axes of the slice: x: 4, y: 4, z: 4, core: 2. Of those that a mesh axis runs over, the one named last changes fastest.
Arguments:
- slip: bfloat16 [128, 32768], P(None, 'leaf'), may hold values from -6 to 6
- to_multipole: bfloat16 [121, 128], replicated, may hold values from -0.5 to 0.5
- up_shift: float32 [2, 121, 121], replicated, may hold values from -0.375 to 0.375
- down_shift: float32 [2, 121, 121], replicated, may hold values from -0.5 to 0.5
- sibling_far: float32 [2, 121, 121], replicated, may hold values from -0.5 to 0.5
- leaf_far: bfloat16 [27, 121, 121], replicated, may hold values from -0.25 to 0.25
- to_stress: bfloat16 [128, 121], replicated, may hold values from -0.125 to 0.125
- near_blocks: bfloat16 [9, 128, 128], replicated, may hold values from -0.1875 to 0.1875
- send_cells: int32 [128, 16384], P('leaf'), may hold values from 0 to 255, as said below
- far_list: int32 [27, 32768], P(None, 'leaf'), may hold values from 0 to 16639, as said below
- near_list: int32 [9, 32768], P(None, 'leaf'), may hold values from 0 to 319, as said below
Outputs:
- stress: float32 [128, 32768], P(None, 'leaf')
The draws below stay inside these ranges and needn't reach their ends.
Inputs may be any that keep to these rules, and one draw needn't show every extreme that they name: `send_cells`: row q holds, in positions d * 128 to (d + 1) * 128 - 1, 128 distinct cells of device q (numbered within that device) listed for receiving device d. `far_list`: an entry v below 256 names a cell of the target's own device. Otherwise v - 256 = q * 128 + s names slot s of device q's list for the target's device, q is not the target's device, s < 128 when q lies within 4 devices of it and s < 32 when it lies farther; in every draw some entry names slot 127 of a device within 4, and some names slot 31 of a farther device. `near_list`: an entry w names the cell w - 32 counted from the first cell of the target's device, so that positions before 0 and from 256 on lie on the neighbouring devices (zeros outside the fault); entry 4 is the target itself.
All inputs are finite; a program needn't handle non-finite values.
Results may differ from the reference program's by a relative error of at most 0.0031.
Values may be sent and summed in bfloat16 or wider, within the bound.
A program may use at most 64 MiB of HBM per device.

```python
import jax
import jax.numpy as jnp
from jax import lax

ELEM = 128
COEF = 121
NEAR = 9
TYPES = 27
NEAR_PEERS = 4
CELLS_DEV = 256
HALO = 32
CAP_NEAR = 128
CAP_FAR = 32
CELLS = 32768
N_LEAF = 128


def let_plan(key):
    base = jax.random.fold_in(key, 4127)
    keys = jax.random.split(base, 5)
    devices_all = N_LEAF
    receiver = jnp.arange(devices_all, dtype=jnp.int32)[:, None]
    sender = jnp.arange(devices_all, dtype=jnp.int32)[None, :]
    apart = jnp.abs(sender - receiver)
    close_count = jax.random.randint(keys[0], (devices_all, devices_all), CAP_NEAR // 4, CAP_NEAR + 1)
    far_count = jax.random.randint(keys[1], (devices_all, devices_all), CAP_FAR // 2, CAP_FAR + 1)
    counts = jnp.where(apart == 0, 0, jnp.where(apart <= NEAR_PEERS, close_count, far_count))
    counts = jnp.where(sender == receiver + 1, CAP_NEAR, counts)
    counts = jnp.where(sender == (receiver + devices_all // 2) % devices_all, CAP_FAR, counts)
    scores = jax.random.randint(keys[2], (devices_all, devices_all, CELLS_DEV), 0, 1 << 20)
    scores = scores * CELLS_DEV + jnp.arange(CELLS_DEV, dtype=jnp.int32)
    chosen = jnp.argsort(scores, axis=-1)[:, :, :CAP_NEAR].astype(jnp.int32)
    send_lists = chosen.reshape(devices_all, devices_all * CAP_NEAR)
    entries = TYPES * CELLS_DEV
    position = jnp.arange(CAP_NEAR, dtype=jnp.int32)
    usable = (position[None, None, :] < counts[:, :, None]).reshape(devices_all, devices_all * CAP_NEAR)
    codes = CELLS_DEV + jnp.arange(devices_all * CAP_NEAR, dtype=jnp.int32)
    ranks = jnp.cumsum(usable.astype(jnp.int32), axis=1) - 1
    place_scores = jax.random.randint(keys[3], (devices_all, entries - 1), 0, 1 << 14)
    place_scores = place_scores * entries + jnp.arange(entries - 1, dtype=jnp.int32)
    places = 1 + jnp.argsort(place_scores, axis=1).astype(jnp.int32)
    targets = jnp.take_along_axis(places, jnp.clip(ranks, 0, entries - 2), axis=1)
    targets = jnp.where(usable, targets, entries)
    own_cells = jax.random.randint(keys[4], (devices_all, entries), 0, CELLS_DEV)
    own_cells = own_cells.at[:, 0].set(0)
    rows = jnp.broadcast_to(receiver, targets.shape)
    filled = own_cells.at[rows, targets].set(jnp.broadcast_to(codes[None, :], targets.shape), mode='drop')
    lists = filled.reshape(devices_all, TYPES, CELLS_DEV).transpose(1, 0, 2).reshape(TYPES, devices_all * CELLS_DEV)
    return (send_lists.astype(jnp.int32), lists.astype(jnp.int32))


def draw_send_cells(key, part):
    return let_plan(key)[0]


def draw_far_list(key, part):
    return let_plan(key)[1]


def draw_near_list(key, part):
    base = jax.random.fold_in(key, 9151)
    cells_here = jnp.arange(CELLS_DEV, dtype=jnp.int32)
    jumps = jax.random.randint(base, (NEAR, N_LEAF, CELLS_DEV), -HALO, HALO + 1)
    kinds = jnp.arange(NEAR, dtype=jnp.int32)[:, None, None]
    jumps = jnp.where(kinds == NEAR // 2, 0, jumps)
    values = cells_here[None, None, :] + HALO + jumps
    values = values.at[0, :, 0].set(0)
    values = values.at[NEAR - 1, :, CELLS_DEV - 1].set(CELLS_DEV + 2 * HALO - 1)
    return values.reshape(NEAR, N_LEAF * CELLS_DEV).astype(jnp.int32)


def level_of(stream_key, extent, cuts, least, largest):
    def one(dim, shards_of):
        steps = jax.random.uniform(jax.random.fold_in(jax.random.fold_in(stream_key, 6), dim), (shards_of,), jnp.float32, least / len(cuts), largest / len(cuts))
        return jnp.repeat(jnp.exp(steps), extent[dim] // shards_of).reshape((-1,) + (1,) * (len(extent) - dim - 1))

    loudness = one(*cuts[0])
    for cut in cuts[1:]:
        loudness = loudness * one(*cut)
    return loudness


def noise(stream_key, dims, spread, bound, pieces=(), kind=jnp.bfloat16):
    values = spread * jax.random.normal(stream_key, dims, jnp.float32)
    if pieces:
        values = values * level_of(stream_key, dims, pieces, -0.22, 0.18)
    return jnp.clip(values, -bound, bound).astype(kind)


def setup_inputs(seed: int = 0) -> dict:
    key_of = jax.random.split(jax.random.key(seed), 12)
    return {
        "slip": noise(key_of[0], (ELEM, CELLS), 1.0, 6.0, ((1, 128),)),
        "to_multipole": noise(key_of[1], (COEF, ELEM), ELEM ** -0.5, 0.5),
        "up_shift": noise(key_of[2], (2, COEF, COEF), (2 * COEF) ** -0.5, 0.375, (), jnp.float32),
        "down_shift": noise(key_of[3], (2, COEF, COEF), COEF ** -0.5, 0.5, (), jnp.float32),
        "sibling_far": noise(key_of[4], (2, COEF, COEF), COEF ** -0.5, 0.5, (), jnp.float32),
        "leaf_far": noise(key_of[5], (TYPES, COEF, COEF), (4 * COEF) ** -0.5, 0.25),
        "to_stress": noise(key_of[6], (ELEM, COEF), (16 * COEF) ** -0.5, 0.125),
        "near_blocks": noise(key_of[7], (NEAR, ELEM, ELEM), (NEAR * ELEM) ** -0.5, 0.1875),
        "send_cells": draw_send_cells(jax.random.fold_in(key_of[11], 71), 0),
        "far_list": draw_far_list(jax.random.fold_in(key_of[11], 71), 0),
        "near_list": draw_near_list(jax.random.fold_in(key_of[11], 71), 0),
    }


def reference(slip, to_multipole, up_shift, down_shift, sibling_far, leaf_far, to_stress, near_blocks, send_cells, far_list, near_list):
    precise = lax.Precision.HIGHEST
    multipole = jnp.dot(to_multipole, slip, preferred_element_type=jnp.float32).astype(jnp.bfloat16)
    heights = CELLS.bit_length() - 1
    aggregates = [multipole.astype(jnp.float32)]
    for height in range(heights - 1):
        below = aggregates[-1]
        aggregates.append(jnp.dot(up_shift[0], below[:, 0::2], precision=precise)
                          + jnp.dot(up_shift[1], below[:, 1::2], precision=precise))
    expansion = jnp.zeros((COEF, 1), jnp.float32)
    for height in range(heights - 1, -1, -1):
        left_part = jnp.dot(down_shift[0], expansion, precision=precise)
        right_part = jnp.dot(down_shift[1], expansion, precision=precise)
        if height >= 1:
            level_sums = aggregates[height]
            left_part = left_part + jnp.dot(sibling_far[0], level_sums[:, 1::2], precision=precise)
            right_part = right_part + jnp.dot(sibling_far[1], level_sums[:, 0::2], precision=precise)
        expansion = jnp.stack([left_part, right_part], axis=-1).reshape(COEF, -1)
    owner = jnp.arange(CELLS, dtype=jnp.int32) // CELLS_DEV
    relative = far_list - CELLS_DEV
    sender = jnp.clip(relative // CAP_NEAR, 0, N_LEAF - 1).astype(jnp.int32)
    position = (relative % CAP_NEAR).astype(jnp.int32)
    flat_lists = send_cells.reshape(-1)
    listed = flat_lists[sender * (N_LEAF * CAP_NEAR) + owner[None, :] * CAP_NEAR + position]
    source = jnp.where(far_list < CELLS_DEV, owner[None, :] * CELLS_DEV + far_list, sender * CELLS_DEV + listed).astype(jnp.int32)
    leaf_sum = jnp.zeros((COEF, CELLS), jnp.float32)
    for kind in range(TYPES):
        leaf_sum = leaf_sum + jnp.dot(leaf_far[kind], jnp.take(multipole, source[kind], axis=1), preferred_element_type=jnp.float32)
    local_exp = (expansion + leaf_sum).astype(jnp.bfloat16)
    padded = jnp.pad(slip, ((0, 0), (HALO, HALO)))
    near_source = (owner[None, :] * CELLS_DEV + near_list).astype(jnp.int32)
    stress = jnp.dot(to_stress, local_exp, preferred_element_type=jnp.float32)
    for kind in range(NEAR):
        stress = stress + jnp.dot(near_blocks[kind], jnp.take(padded, near_source[kind], axis=1), preferred_element_type=jnp.float32)
    return stress
```

```python
import functools

import jax
import jax.numpy as jnp
from jax import lax
from jax.experimental import pallas as pl
from jax.experimental.pallas import tpu as pltpu
from jax.sharding import PartitionSpec as P

N = 128
CELLS = 256
COEF = 121
FAR = 32
NEARCAP = 128
HALO = 32
FIRST = 5
LAST = 123
f32 = jnp.float32
bf16 = jnp.bfloat16
MESH = pl.DeviceIdType.MESH
NT = (((1,), (1,)), ((), ()))
TN = (((0,), (0,)), ((), ()))


def exchange(slip_ref, wm_ref, send_ref, mt_ref, near_ref, far_ref, halo_ref,
             wp, sendbuf, nearbuf, halobuf, send_sem, far_sem, near_sem, halo_sem):
    me = lax.axis_index("leaf")
    barrier = pltpu.get_barrier_semaphore()

    def hello(k, carry):
        pl.semaphore_signal(barrier, inc=1, device_id=(lax.rem(me + k, N),), device_id_type=MESH)
        return carry

    lax.fori_loop(1, N, hello, 0)
    wp[...] = jnp.zeros_like(wp)
    wp[0:COEF, :] = wm_ref[...]
    mt = lax.dot_general(slip_ref[...], wp[...], (((0,), (1,)), ((), ())), preferred_element_type=f32).astype(bf16)
    mt_ref[...] = mt
    cell = lax.broadcasted_iota(jnp.int32, (HALO, CELLS), 1)
    row = lax.broadcasted_iota(jnp.int32, (HALO, CELLS), 0)
    for side in range(2):
        pick = (cell == row + (CELLS - HALO) * (1 - side)).astype(f32).astype(bf16)
        halobuf[side] = lax.dot_general(pick, slip_ref[...], NT, preferred_element_type=f32).astype(bf16)
    lists = pltpu.roll(send_ref[...].astype(f32).T, lax.rem(N - me, N), 1)
    lane = lax.broadcasted_iota(jnp.int32, (NEARCAP, CELLS), 1).astype(f32)
    near_at = (1, 2, 3, 4, 124, 125, 126, 127)
    for i, k in enumerate(near_at):
        hot = (lists[:, k:k + 1] == lane).astype(f32).astype(bf16)
        nearbuf[i] = jnp.dot(hot, mt, preferred_element_type=f32).astype(bf16)
    for k in range(FIRST, LAST + 1):
        hot = (lists[0:FAR, k:k + 1] == lane[0:FAR]).astype(f32).astype(bf16)
        sendbuf[k] = jnp.dot(hot, mt, preferred_element_type=f32).astype(bf16)
    pl.semaphore_wait(barrier, N - 1)

    def far_copy(k):
        return pltpu.make_async_remote_copy(
            src_ref=sendbuf.at[k], dst_ref=far_ref.at[me], send_sem=send_sem.at[0], recv_sem=far_sem,
            device_id=(lax.rem(me + k, N),), device_id_type=MESH)

    def near_copy(i, k):
        return pltpu.make_async_remote_copy(
            src_ref=nearbuf.at[i], dst_ref=near_ref.at[i], send_sem=send_sem.at[1], recv_sem=near_sem,
            device_id=(lax.rem(me + k, N),), device_id_type=MESH)

    def halo_copy(side):
        return pltpu.make_async_remote_copy(
            src_ref=halobuf.at[side], dst_ref=halo_ref.at[side], send_sem=send_sem.at[2], recv_sem=halo_sem,
            device_id=(lax.rem(me + (1, N - 1)[side], N),), device_id_type=MESH)

    for side in range(2):
        halo_copy(side).start()
    for i, k in enumerate(near_at):
        near_copy(i, k).start()

    def go(i, carry):
        far_copy(FIRST + lax.rem(i * 37, LAST - FIRST + 1)).start()
        return carry

    lax.fori_loop(0, LAST - FIRST + 1, go, 0)
    count = LAST - FIRST + 1
    pltpu.make_async_copy(halobuf, halobuf, send_sem.at[2]).wait()
    pltpu.make_async_copy(halobuf, halo_ref, halo_sem).wait()
    pltpu.make_async_copy(nearbuf, nearbuf, send_sem.at[1]).wait()
    pltpu.make_async_copy(nearbuf, near_ref, near_sem).wait()
    pltpu.make_async_copy(sendbuf.at[0:count], sendbuf.at[0:count], send_sem.at[0]).wait()
    pltpu.make_async_copy(sendbuf.at[0:count], sendbuf.at[0:count], far_sem).wait()


def call_exchange(slip, to_multipole, send):
    vm = pl.BlockSpec(memory_space=pltpu.VMEM)
    return pl.pallas_call(
        exchange,
        out_shape=(
            jax.ShapeDtypeStruct((CELLS, 128), bf16),
            jax.ShapeDtypeStruct((8, NEARCAP, 128), bf16),
            jax.ShapeDtypeStruct((N, FAR, 128), bf16),
            jax.ShapeDtypeStruct((2, HALO, 128), bf16),
        ),
        in_specs=[vm] * 3,
        out_specs=(vm,) * 4,
        scratch_shapes=[
            pltpu.VMEM((128, 128), bf16),
            pltpu.VMEM((N, FAR, 128), bf16),
            pltpu.VMEM((8, NEARCAP, 128), bf16),
            pltpu.VMEM((2, HALO, 128), bf16),
            pltpu.SemaphoreType.DMA((3,)),
            pltpu.SemaphoreType.DMA,
            pltpu.SemaphoreType.DMA,
            pltpu.SemaphoreType.DMA,
        ],
        compiler_params=pltpu.CompilerParams(collective_id=0, has_side_effects=True),
        name="exchange",
    )(slip, to_multipole, send.reshape(N, NEARCAP))


def swapped(block, axis, stride):
    count = lax.axis_size(axis)
    route = []
    for low in range(count):
        high = low | 1 << stride
        if high != low and high < count:
            route += [(low, high), (high, low)]
    return lax.ppermute(block, axis, route)


def pair_up(up_shift, lower, upper):
    precise = lax.Precision.HIGHEST
    return jnp.dot(up_shift[0], lower, precision=precise) + jnp.dot(up_shift[1], upper, precision=precise)


def body(slip, to_multipole, up_shift, down_shift, sibling_far, leaf_far, to_stress, near_blocks,
         send_cells, far_list, near_list):
    precise = lax.Precision.HIGHEST
    me = lax.axis_index("leaf")
    mt, near_rows, far_rows, halos = call_exchange(slip, to_multipole, send_cells)
    multipole = mt[:, :COEF].T
    left = jnp.where(me > 0, halos[0].T, 0)
    right = jnp.where(me < N - 1, halos[1].T, 0)
    extended = jnp.concatenate([left, slip, right], axis=1)
    near_cols = jnp.take(extended, near_list.reshape(-1), axis=1, mode="clip").reshape(128, 9, CELLS)
    near_part = jnp.einsum("kij,jkc->ic", near_blocks, near_cols, preferred_element_type=f32)
    table = jnp.concatenate([mt, near_rows.reshape(-1, 128), far_rows.reshape(-1, 128)], axis=0)
    rel = far_list - CELLS
    sender = rel // NEARCAP
    slot = rel % NEARCAP
    off = (me - sender) % N
    near_i = jnp.where(off <= 4, off - 1, off - 120)
    is_near = (off <= 4) | (off >= 124)
    row = jnp.where(far_list < CELLS, far_list,
                    jnp.where(is_near, CELLS + near_i * NEARCAP + slot, CELLS + 8 * NEARCAP + sender * FAR + slot))
    cols = jnp.take(table, row.reshape(-1), axis=0, mode="clip").reshape(27, CELLS, 128)[:, :, :COEF]
    leaf_sum = jnp.einsum("tij,tcj->ic", leaf_far, cols, preferred_element_type=f32)
    aggregates = [multipole.astype(f32)]
    for height in range(8):
        below = aggregates[-1]
        aggregates.append(pair_up(up_shift, below[:, 0::2], below[:, 1::2]))
    current = aggregates[-1]
    siblings = []
    for bit in range(7):
        partner = swapped(current, "leaf", bit)
        siblings.append(partner)
        if bit < 6:
            branch = me >> bit & 1
            current = pair_up(up_shift, jnp.where(branch == 0, current, partner),
                              jnp.where(branch == 0, partner, current))
    expansion = jnp.zeros((COEF, 1), f32)
    for bit in reversed(range(7)):
        branch = me >> bit & 1
        down_pick = lax.dynamic_index_in_dim(down_shift, branch, 0, keepdims=False)
        far_pick = lax.dynamic_index_in_dim(sibling_far, branch, 0, keepdims=False)
        expansion = jnp.dot(down_pick, expansion, precision=precise) + jnp.dot(far_pick, siblings[bit], precision=precise)
    for height in reversed(range(8)):
        a = jnp.dot(down_shift[0], expansion, precision=precise)
        b = jnp.dot(down_shift[1], expansion, precision=precise)
        if height >= 1:
            sums = aggregates[height]
            a = a + jnp.dot(sibling_far[0], sums[:, 1::2], precision=precise)
            b = b + jnp.dot(sibling_far[1], sums[:, 0::2], precision=precise)
        expansion = jnp.stack([a, b], axis=-1).reshape(COEF, -1)
    local_exp = (expansion + leaf_sum).astype(bf16)
    return jnp.dot(to_stress, local_exp, preferred_element_type=f32) + near_part


def solution(mesh):
    cut = P(None, "leaf")
    return jax.shard_map(body, mesh=mesh,
                         in_specs=(cut, P(), P(), P(), P(), P(), P(), P(), P("leaf", None), cut, cut),
                         out_specs=cut, check_vma=False)
```

```python
import jax
import jax.numpy as jnp
from jax import lax
from jax.experimental import pallas as pl
from jax.experimental.pallas import tpu as pltpu
from jax.sharding import PartitionSpec as P

N = 128
CELLS = 256
COEF = 121
ELEM = 128
FAR = 32
SLOTS = 128
HALO = 32
KINDS = 27
NEAR = 9
CLOSE = (1, 2, 3, 4, 124, 125, 126, 127)
FIRST = 5
COUNT = 119
ORDER = tuple(FIRST + i * 37 % COUNT for i in range(COUNT))
GROUP = 8
OWN_AT, CLOSE_AT, FAR_AT = 0, CELLS, CELLS + 8 * SLOTS
ROWS = FAR_AT + N * FAR
LEVEL_AT = (None, 0, 128, 192, 224, 240, 248, 252, 254)
BLOCK_AT = (0, 128, 192, 224, 240, 248, 252)
f32 = jnp.float32
bf16 = jnp.bfloat16
i32 = jnp.int32
MESH = pl.DeviceIdType.MESH
NT = (((1,), (1,)), ((), ()))
TN = (((0,), (0,)), ((), ()))


def mm(a, b):
    return jnp.dot(a, b, preferred_element_type=f32)


def split(x):
    high = x.astype(bf16)
    return high, (x - high.astype(f32)).astype(bf16)


def tripled(x):
    high, low = split(x)
    return jnp.concatenate([high, high, low], axis=1)


def onehot(index, count, axis, shape):
    return (index == lax.broadcasted_iota(i32, shape, axis)).astype(f32).astype(bf16)


def step_kernel(slip_hbm, wm_hbm, up_hbm, down_hbm, sib_hbm, leaf_hbm, ts_hbm, blocks_hbm, send_hbm, far_hbm, near_hbm,
                out_ref,
                slip, wm, up, down, sib, leaf, ts, blocks, send, far_list, near_list,
                wp, tsp, pad, up3, down3, sib3, leafp,
                sendbuf, closebuf, closein, halobuf, haloin, farin, rootbuf, roots,
                agg, blockagg, sibterm0, sibterm1, local, near_acc, indices, table, smem,
                load_sem, send_sem, far_sem, close_sem, halo_sem, root_sem, smem_sem):
    me = lax.axis_index("leaf")
    pairs = ((slip_hbm, slip), (wm_hbm, wm), (send_hbm, send), (up_hbm, up), (down_hbm, down), (sib_hbm, sib),
             (far_hbm, far_list), (near_hbm, near_list), (blocks_hbm, blocks), (ts_hbm, ts), (leaf_hbm, leaf))
    loads = [pltpu.make_async_copy(a, b, load_sem.at[i]) for i, (a, b) in enumerate(pairs)]
    for load in loads:
        load.start()
    barrier = pltpu.get_barrier_semaphore()

    def hello(k, carry):
        pl.semaphore_signal(barrier, inc=1, device_id=(lax.rem(me + k, N),), device_id_type=MESH)
        return carry

    lax.fori_loop(1, N, hello, 0)

    wp[...] = jnp.zeros_like(wp)
    loads[0].wait()
    loads[1].wait()
    wp[0:COEF, :] = wm[...]
    mt = lax.dot_general(slip[...], wp[...], (((0,), (1,)), ((), ())), preferred_element_type=f32).astype(bf16)
    for side in range(2):
        pick = onehot(lax.broadcasted_iota(i32, (HALO, CELLS), 0) + (CELLS - HALO) * (1 - side), CELLS, 1, (HALO, CELLS))
        halobuf[side] = lax.dot_general(pick, slip[...], NT, preferred_element_type=f32).astype(bf16)

    loads[2].wait()
    lists = pltpu.roll(send[...].astype(f32).T, lax.rem(N - me, N), 1)
    lane = lax.broadcasted_iota(i32, (SLOTS, CELLS), 1).astype(f32)

    def peer(k):
        return (lax.rem(me + k, N),)

    def far_copy(k):
        return pltpu.make_async_remote_copy(
            src_ref=sendbuf.at[k], dst_ref=farin.at[me], send_sem=send_sem.at[0], recv_sem=far_sem,
            device_id=peer(k), device_id_type=MESH)

    def close_copy(i):
        return pltpu.make_async_remote_copy(
            src_ref=closebuf.at[i], dst_ref=closein.at[i], send_sem=send_sem.at[1], recv_sem=close_sem,
            device_id=peer(CLOSE[i]), device_id_type=MESH)

    def halo_copy(side):
        return pltpu.make_async_remote_copy(
            src_ref=halobuf.at[side], dst_ref=haloin.at[side], send_sem=send_sem.at[2], recv_sem=halo_sem,
            device_id=peer((1, N - 1)[side]), device_id_type=MESH)

    def root_copy(k):
        return pltpu.make_async_remote_copy(
            src_ref=rootbuf, dst_ref=roots.at[me], send_sem=send_sem.at[3], recv_sem=root_sem,
            device_id=peer(k), device_id_type=MESH)

    def fill(ks):
        for k in ks:
            hot = (lists[0:FAR, k:k + 1] == lane[0:FAR]).astype(f32).astype(bf16)
            sendbuf[k] = mm(hot, mt).astype(bf16)

    groups = [ORDER[i:i + GROUP] for i in range(0, COUNT, GROUP)]
    for i, k in enumerate(CLOSE):
        hot = (lists[:, k:k + 1] == lane).astype(f32).astype(bf16)
        closebuf[i] = mm(hot, mt).astype(bf16)
    fill(groups[0])
    pl.semaphore_wait(barrier, N - 1)
    for side in range(2):
        halo_copy(side).start()
    for i in range(8):
        close_copy(i).start()
    half = len(groups) // 2
    for g in range(half):
        fill(groups[g + 1])
        for k in groups[g]:
            far_copy(k).start()

    pad[...] = jnp.zeros_like(pad)

    def padded_t(ref, s):
        pad[0:COEF, 0:COEF] = ref[:, s, :]
        return split(pad[...].T)

    loads[3].wait()
    for s in range(2):
        high, low = padded_t(up, s)
        up3[s * 128:s * 128 + 128, :] = high
        up3[256 + s * 128:256 + s * 128 + 128, :] = low
        up3[512 + s * 128:512 + s * 128 + 128, :] = high

    def pair_up(ref, at, count):
        pair = jnp.concatenate([ref[pl.ds(at, count, stride=2), :], ref[pl.ds(at + 1, count, stride=2), :]], axis=1)
        return mm(tripled(pair), up3[...])

    table[OWN_AT:OWN_AT + CELLS, :] = mt.astype(f32)
    agg[248:256, :] = jnp.zeros((8, 128), f32)
    agg[0:128, :] = pair_up(table, OWN_AT, 128)
    for level in range(1, 8):
        count = 128 >> level
        agg[pl.ds(LEVEL_AT[level + 1], count), :] = pair_up(agg, LEVEL_AT[level], count)
    root = agg[pl.ds(LEVEL_AT[8], 1), :]
    rootbuf[...] = root
    roots[me] = root

    for g in range(half, len(groups)):
        if g + 1 < len(groups):
            fill(groups[g + 1])
        for k in groups[g]:
            far_copy(k).start()
        if g == half:
            def tell(k, carry):
                root_copy(k).start()
                return carry
            lax.fori_loop(1, N, tell, 0)

    for load, ref, ref3 in ((loads[4], down, down3), (loads[5], sib, sib3)):
        load.wait()
        for s in range(2):
            high, low = padded_t(ref, s)
            ref3[0:128, s * 128:s * 128 + 128] = high
            ref3[128:256, s * 128:s * 128 + 128] = low
            ref3[256:384, s * 128:s * 128 + 128] = high
    sibs = mm(tripled(agg[...]), sib3[...])
    sibterm0[...] = sibs[:, 0:128]
    sibterm1[...] = sibs[:, 128:256]

    loads[6].wait()
    entry = far_list[...]
    rel = entry - CELLS
    sender = rel // SLOTS
    slot = rel - sender * SLOTS
    off = (me - sender) & (N - 1)
    close = jnp.where(off <= 4, off - 1, off - 120)
    is_close = (off <= 4) | (off >= 124)
    row = jnp.where(is_close, CLOSE_AT + close * SLOTS + slot, FAR_AT + sender * FAR + slot)
    indices[...] = jnp.where(entry < CELLS, entry, row)
    to_smem = pltpu.make_async_copy(indices, smem, smem_sem)
    to_smem.start()

    loads[7].wait()
    loads[8].wait()
    loads[9].wait()
    pltpu.make_async_copy(halobuf, haloin, halo_sem).wait()
    left = jnp.where(me > 0, haloin[0].astype(f32), 0.0)
    right = jnp.where(me < N - 1, haloin[1].astype(f32), 0.0)
    edge = jnp.concatenate([left, right], axis=0).T.astype(bf16)
    own = slip[...]
    near_acc[...] = jnp.zeros_like(near_acc)
    for k in range(NEAR):
        w = near_list[k:k + 1, :]
        at = jnp.where(w < HALO, w + CELLS, jnp.where(w < HALO + CELLS, w - HALO, w))
        hot = onehot(at, 0, 0, (CELLS + 2 * HALO, CELLS))
        cols = mm(own, hot[0:CELLS]) + mm(edge, hot[CELLS:])
        near_acc[...] += mm(blocks[k], cols.astype(bf16))
    tsp[...] = jnp.zeros_like(tsp)
    tsp[:, 0:COEF] = ts[...]

    pltpu.make_async_copy(roots.at[0:N - 1], roots.at[0:N - 1], root_sem).wait()
    blockagg[0:N, :] = roots[...].reshape(N, 128)
    for bit in range(6):
        count = 64 >> bit
        blockagg[pl.ds(BLOCK_AT[bit + 1], count), :] = pair_up(blockagg, BLOCK_AT[bit], count)
    branch = [(me >> bit) & 1 for bit in range(7)]
    rows = [blockagg[pl.ds(BLOCK_AT[bit] + ((me >> bit) ^ 1), 1), :] for bit in range(7)]
    terms = mm(tripled(jnp.concatenate(rows + [rows[0]], axis=0)), sib3[...])
    expansion = jnp.zeros((8, 128), f32)
    for bit in reversed(range(7)):
        both = jnp.broadcast_to(terms[bit:bit + 1, :], (8, 256))
        if bit < 6:
            both = both + mm(tripled(expansion), down3[...])
        expansion = jnp.where(branch[bit] == 0, both[:, 0:128], both[:, 128:256])

    local[0:8, :] = jnp.zeros((8, 128), f32)
    for level in reversed(range(8)):
        count = 128 >> level
        both = mm(tripled(expansion), down3[...])
        low, high = both[0:count, 0:128], both[0:count, 128:256]
        if level >= 1:
            at = LEVEL_AT[level]
            low = low + sibterm0[pl.ds(at + 1, count, stride=2), :]
            high = high + sibterm1[pl.ds(at, count, stride=2), :]
        local[pl.ds(0, count, stride=2), :] = low
        local[pl.ds(1, count, stride=2), :] = high
        expansion = local[0:max(2 * count, 8), :]

    leafp[...] = jnp.zeros_like(leafp)
    loads[10].wait()
    for t in range(KINDS):
        leafp[t, 0:COEF, 0:COEF] = leaf[t]

    pltpu.make_async_copy(closebuf, closein, close_sem).wait()
    for i in range(8):
        table[CLOSE_AT + i * SLOTS:CLOSE_AT + (i + 1) * SLOTS, :] = closein[i].astype(f32)
    to_smem.wait()
    pltpu.make_async_copy(farin.at[0:COUNT], farin.at[0:COUNT], far_sem).wait()

    def widen(q, carry):
        for j in range(4):
            table[pl.ds(pl.multiple_of(FAR_AT + (q * 4 + j) * FAR, FAR), FAR), :] = farin[q * 4 + j].astype(f32)
        return carry

    lax.fori_loop(0, N // 4, widen, 0)

    sub = lax.broadcasted_iota(i32, (8, 128), 0)
    total = local[...]
    for t in range(KINDS):
        parts = []
        for b in range(CELLS // 8):
            v = jnp.broadcast_to(table[pl.ds(smem[t, b * 8], 1), :], (8, 128))
            for j in range(1, 8):
                r = jnp.broadcast_to(table[pl.ds(smem[t, b * 8 + j], 1), :], (8, 128))
                v = jnp.where(sub == j, r, v)
            parts.append(v)
        rows = jnp.concatenate(parts, axis=0).astype(bf16)
        total = total + lax.dot_general(rows, leafp[t], NT, preferred_element_type=f32)
    stress = lax.dot_general(tsp[...], total.astype(bf16), NT, preferred_element_type=f32)
    out_ref[...] = stress + near_acc[...]

    pltpu.make_async_copy(halobuf, halobuf, send_sem.at[2]).wait()
    pltpu.make_async_copy(closebuf, closebuf, send_sem.at[1]).wait()
    pltpu.make_async_copy(roots.at[0:N - 1], roots.at[0:N - 1], send_sem.at[3]).wait()
    pltpu.make_async_copy(sendbuf.at[0:COUNT], sendbuf.at[0:COUNT], send_sem.at[0]).wait()


def body(slip, to_multipole, up_shift, down_shift, sibling_far, leaf_far, to_stress, near_blocks,
         send_cells, far_list, near_list):
    up_shift, down_shift, sibling_far = (x.transpose(1, 0, 2) for x in (up_shift, down_shift, sibling_far))
    args = (slip, to_multipole, up_shift, down_shift, sibling_far, leaf_far, to_stress, near_blocks,
            send_cells.reshape(N, SLOTS), far_list, near_list)
    anywhere = pl.BlockSpec(memory_space=pl.ANY)
    return pl.pallas_call(
        step_kernel,
        out_shape=jax.ShapeDtypeStruct((ELEM, CELLS), f32),
        in_specs=[anywhere] * len(args),
        out_specs=pl.BlockSpec(memory_space=pltpu.VMEM),
        scratch_shapes=[pltpu.VMEM(a.shape, a.dtype) for a in args] + [
            pltpu.VMEM((128, 128), bf16),
            pltpu.VMEM((128, 128), bf16),
            pltpu.VMEM((128, 128), f32),
            pltpu.VMEM((768, 128), bf16),
            pltpu.VMEM((384, 256), bf16),
            pltpu.VMEM((384, 256), bf16),
            pltpu.VMEM((KINDS, 128, 128), bf16),
            pltpu.VMEM((N, FAR, 128), bf16),
            pltpu.VMEM((8, SLOTS, 128), bf16),
            pltpu.VMEM((8, SLOTS, 128), bf16),
            pltpu.VMEM((2, HALO, ELEM), bf16),
            pltpu.VMEM((2, HALO, ELEM), bf16),
            pltpu.VMEM((N, FAR, 128), bf16),
            pltpu.VMEM((1, 128), f32),
            pltpu.VMEM((N, 1, 128), f32),
            pltpu.VMEM((256, 128), f32),
            pltpu.VMEM((256, 128), f32),
            pltpu.VMEM((256, 128), f32),
            pltpu.VMEM((256, 128), f32),
            pltpu.VMEM((256, 128), f32),
            pltpu.VMEM((ELEM, CELLS), f32),
            pltpu.VMEM((KINDS, CELLS), i32),
            pltpu.VMEM((ROWS, 128), f32),
            pltpu.SMEM((KINDS, CELLS), i32),
            pltpu.SemaphoreType.DMA((len(args),)),
            pltpu.SemaphoreType.DMA((4,)),
            pltpu.SemaphoreType.DMA,
            pltpu.SemaphoreType.DMA,
            pltpu.SemaphoreType.DMA,
            pltpu.SemaphoreType.DMA,
            pltpu.SemaphoreType.DMA,
        ],
        compiler_params=pltpu.CompilerParams(collective_id=0, has_side_effects=True),
        name="step",
    )(*args)


def solution(mesh):
    cut = P(None, "leaf")
    return jax.shard_map(body, mesh=mesh,
                         in_specs=(cut, P(), P(), P(), P(), P(), P(), P(), P("leaf", None), cut, cut),
                         out_specs=cut, check_vma=False)
```

```python
import jax
import jax.numpy as jnp
from jax import lax
from jax.experimental import pallas as pl
from jax.experimental.pallas import tpu as pltpu
from jax.sharding import PartitionSpec as P

N = 128
CELLS = 256
COEF = 121
ELEM = 128
FAR = 32
SLOTS = 128
HALO = 32
KINDS = 27
NEAR = 9
CLOSE = (1, 2, 3, 4, 124, 125, 126, 127)
FIRST = 5
COUNT = 119


def hops(k):
    return sum(min(k // d % 4, 4 - k // d % 4) for d in (32, 8, 2))


ORDER = tuple(sorted((FIRST + i * 37 % COUNT for i in range(COUNT)), key=lambda k: -hops(k)))
ROOTS_AFTER = 12
CUTS = (0, 30, 60, 90, 105, COUNT)
CLASS = {k: j for j in range(len(CUTS) - 1) for k in ORDER[CUTS[j]:CUTS[j + 1]]}
CLOSE_AFTER = 60
OWN_AT, CLOSE_AT, FAR_AT = 0, CELLS, CELLS + 8 * SLOTS
ROWS = FAR_AT + N * FAR
LEVEL_AT = (None, 0, 128, 192, 224, 240, 248, 252, 254)
BLOCK_AT = (0, 128, 192, 224, 240, 248, 252)
f32 = jnp.float32
bf16 = jnp.bfloat16
i32 = jnp.int32
MESH = pl.DeviceIdType.MESH
NT = (((1,), (1,)), ((), ()))
TN = (((0,), (0,)), ((), ()))


def mm(a, b):
    return jnp.dot(a, b, preferred_element_type=f32)


def split(x):
    high = x.astype(bf16)
    return high, (x - high.astype(f32)).astype(bf16)


def tripled(x):
    high, low = split(x)
    return jnp.concatenate([high, high, low], axis=1)


def onehot(index, count, axis, shape):
    return (index == lax.broadcasted_iota(i32, shape, axis)).astype(f32).astype(bf16)


def step_kernel(slip_hbm, wm_hbm, up_hbm, down_hbm, sib_hbm, leaf_hbm, ts_hbm, blocks_hbm, send_hbm, far_hbm, near_hbm,
                out_ref,
                slip, wm, up, down, sib, leaf, ts, blocks, send, far_list, near_list,
                wp, tsp, pad, up3, down3, sib3, leafp,
                sendbuf, closebuf, closein, halobuf, haloin, farin, rootbuf, roots,
                agg, blockagg, sibterm0, sibterm1, local, near_acc, indices, table, smem,
                load_sem, send_sem, far_sem, close_sem, halo_sem, root_sem, smem_sem):
    me = lax.axis_index("leaf")
    pairs = ((slip_hbm, slip), (wm_hbm, wm), (send_hbm, send), (up_hbm, up), (down_hbm, down), (sib_hbm, sib),
             (far_hbm, far_list), (near_hbm, near_list), (blocks_hbm, blocks), (ts_hbm, ts), (leaf_hbm, leaf))
    loads = [pltpu.make_async_copy(a, b, load_sem.at[i]) for i, (a, b) in enumerate(pairs)]
    for load in loads:
        load.start()
    barrier = pltpu.get_barrier_semaphore()

    def hello(k, carry):
        pl.semaphore_signal(barrier, inc=1, device_id=(lax.rem(me + k, N),), device_id_type=MESH)
        return carry

    lax.fori_loop(1, N, hello, 0)

    wp[...] = jnp.zeros_like(wp)
    loads[0].wait()
    loads[1].wait()
    wp[0:COEF, :] = wm[...]
    mt = lax.dot_general(slip[...], wp[...], (((0,), (1,)), ((), ())), preferred_element_type=f32).astype(bf16)
    for side in range(2):
        pick = onehot(lax.broadcasted_iota(i32, (HALO, CELLS), 0) + (CELLS - HALO) * (1 - side), CELLS, 1, (HALO, CELLS))
        halobuf[side] = lax.dot_general(pick, slip[...], NT, preferred_element_type=f32).astype(bf16)

    loads[2].wait()
    lists = pltpu.roll(send[...].astype(f32).T, lax.rem(N - me, N), 1)
    lane = lax.broadcasted_iota(i32, (SLOTS, CELLS), 1).astype(f32)

    def peer(k):
        return (lax.rem(me + k, N),)

    def far_copy(k):
        return pltpu.make_async_remote_copy(
            src_ref=sendbuf.at[k], dst_ref=farin.at[k], send_sem=send_sem.at[0], recv_sem=far_sem.at[CLASS[k]],
            device_id=peer(k), device_id_type=MESH)

    def close_copy(i):
        return pltpu.make_async_remote_copy(
            src_ref=closebuf.at[i], dst_ref=closein.at[i], send_sem=send_sem.at[1], recv_sem=close_sem,
            device_id=peer(CLOSE[i]), device_id_type=MESH)

    def halo_copy(side):
        return pltpu.make_async_remote_copy(
            src_ref=halobuf.at[side], dst_ref=haloin.at[side], send_sem=send_sem.at[2], recv_sem=halo_sem,
            device_id=peer((1, N - 1)[side]), device_id_type=MESH)

    def root_copy(k):
        return pltpu.make_async_remote_copy(
            src_ref=rootbuf, dst_ref=roots.at[me], send_sem=send_sem.at[3], recv_sem=root_sem,
            device_id=peer(k), device_id_type=MESH)

    def fill(ks):
        for k in ks:
            hot = (lists[0:FAR, k:k + 1] == lane[0:FAR]).astype(f32).astype(bf16)
            sendbuf[k] = mm(hot, mt).astype(bf16)

    for i, k in enumerate(CLOSE):
        hot = (lists[:, k:k + 1] == lane).astype(f32).astype(bf16)
        closebuf[i] = mm(hot, mt).astype(bf16)
    fill(ORDER)

    pad[...] = jnp.zeros_like(pad)

    def padded_t(ref, s):
        pad[0:COEF, 0:COEF] = ref[:, s, :]
        return split(pad[...].T)

    loads[3].wait()
    for s in range(2):
        high, low = padded_t(up, s)
        up3[s * 128:s * 128 + 128, :] = high
        up3[256 + s * 128:256 + s * 128 + 128, :] = low
        up3[512 + s * 128:512 + s * 128 + 128, :] = high

    def pair_up(ref, at, count):
        pair = jnp.concatenate([ref[pl.ds(at, count, stride=2), :], ref[pl.ds(at + 1, count, stride=2), :]], axis=1)
        return mm(tripled(pair), up3[...])

    table[OWN_AT:OWN_AT + CELLS, :] = mt.astype(f32)
    agg[248:256, :] = jnp.zeros((8, 128), f32)
    agg[0:128, :] = pair_up(table, OWN_AT, 128)
    for level in range(1, 8):
        count = 128 >> level
        agg[pl.ds(LEVEL_AT[level + 1], count), :] = pair_up(agg, LEVEL_AT[level], count)
    root = agg[pl.ds(LEVEL_AT[8], 1), :]
    rootbuf[...] = root
    roots[me] = root

    pl.semaphore_wait(barrier, N - 1)

    def tell(k, carry):
        root_copy(k).start()
        return carry

    for i in range(COUNT + 1):
        if i == 10:
            for side in range(2):
                halo_copy(side).start()
        if i % 12 == 11 and i // 12 < 8:
            close_copy(i // 12).start()
        if i == ROOTS_AFTER:
            lax.fori_loop(1, N, tell, 0)
        if i < COUNT:
            far_copy(ORDER[i]).start()

    for load, ref, ref3 in ((loads[4], down, down3), (loads[5], sib, sib3)):
        load.wait()
        for s in range(2):
            high, low = padded_t(ref, s)
            ref3[0:128, s * 128:s * 128 + 128] = high
            ref3[128:256, s * 128:s * 128 + 128] = low
            ref3[256:384, s * 128:s * 128 + 128] = high
    sibs = mm(tripled(agg[...]), sib3[...])
    sibterm0[...] = sibs[:, 0:128]
    sibterm1[...] = sibs[:, 128:256]

    loads[6].wait()
    entry = far_list[...]
    rel = entry - CELLS
    sender = rel // SLOTS
    slot = rel - sender * SLOTS
    off = (me - sender) & (N - 1)
    close = jnp.where(off <= 4, off - 1, off - 120)
    is_close = (off <= 4) | (off >= 124)
    row = jnp.where(is_close, CLOSE_AT + close * SLOTS + slot, FAR_AT + off * FAR + slot)
    indices[...] = jnp.where(entry < CELLS, entry, row)
    to_smem = pltpu.make_async_copy(indices, smem, smem_sem)
    to_smem.start()

    loads[7].wait()
    loads[8].wait()
    loads[9].wait()
    pltpu.make_async_copy(halobuf, haloin, halo_sem).wait()
    left = jnp.where(me > 0, haloin[0].astype(f32), 0.0)
    right = jnp.where(me < N - 1, haloin[1].astype(f32), 0.0)
    edge = jnp.concatenate([left, right], axis=0).T.astype(bf16)
    own = slip[...]
    near_acc[...] = jnp.zeros_like(near_acc)
    for k in range(NEAR):
        w = near_list[k:k + 1, :]
        at = jnp.where(w < HALO, w + CELLS, jnp.where(w < HALO + CELLS, w - HALO, w))
        hot = onehot(at, 0, 0, (CELLS + 2 * HALO, CELLS))
        cols = mm(own, hot[0:CELLS]) + mm(edge, hot[CELLS:])
        near_acc[...] += mm(blocks[k], cols.astype(bf16))
    tsp[...] = jnp.zeros_like(tsp)
    tsp[:, 0:COEF] = ts[...]

    pltpu.make_async_copy(roots.at[0:N - 1], roots.at[0:N - 1], root_sem).wait()
    blockagg[0:N, :] = roots[...].reshape(N, 128)
    for bit in range(6):
        count = 64 >> bit
        blockagg[pl.ds(BLOCK_AT[bit + 1], count), :] = pair_up(blockagg, BLOCK_AT[bit], count)
    branch = [(me >> bit) & 1 for bit in range(7)]
    rows = [blockagg[pl.ds(BLOCK_AT[bit] + ((me >> bit) ^ 1), 1), :] for bit in range(7)]
    terms = mm(tripled(jnp.concatenate(rows + [rows[0]], axis=0)), sib3[...])
    expansion = jnp.zeros((8, 128), f32)
    for bit in reversed(range(7)):
        both = jnp.broadcast_to(terms[bit:bit + 1, :], (8, 256))
        if bit < 6:
            both = both + mm(tripled(expansion), down3[...])
        expansion = jnp.where(branch[bit] == 0, both[:, 0:128], both[:, 128:256])

    local[0:8, :] = jnp.zeros((8, 128), f32)
    for level in reversed(range(8)):
        count = 128 >> level
        both = mm(tripled(expansion), down3[...])
        low, high = both[0:count, 0:128], both[0:count, 128:256]
        if level >= 1:
            at = LEVEL_AT[level]
            low = low + sibterm0[pl.ds(at + 1, count, stride=2), :]
            high = high + sibterm1[pl.ds(at, count, stride=2), :]
        local[pl.ds(0, count, stride=2), :] = low
        local[pl.ds(1, count, stride=2), :] = high
        expansion = local[0:max(2 * count, 8), :]

    leafp[...] = jnp.zeros_like(leafp)
    loads[10].wait()
    for t in range(KINDS):
        leafp[t, 0:COEF, 0:COEF] = leaf[t]

    pltpu.make_async_copy(closebuf, closein, close_sem).wait()
    for i in range(8):
        table[CLOSE_AT + i * SLOTS:CLOSE_AT + (i + 1) * SLOTS, :] = closein[i].astype(f32)
    to_smem.wait()
    for j in range(len(CUTS) - 1):
        count = CUTS[j + 1] - CUTS[j]
        pltpu.make_async_copy(farin.at[0:count], farin.at[0:count], far_sem.at[j]).wait()
        for k in ORDER[CUTS[j]:CUTS[j + 1]]:
            table[FAR_AT + k * FAR:FAR_AT + (k + 1) * FAR, :] = farin[k].astype(f32)

    sub = lax.broadcasted_iota(i32, (8, 128), 0)
    total = local[...]
    for t in range(KINDS):
        parts = []
        for b in range(CELLS // 8):
            v = jnp.broadcast_to(table[pl.ds(smem[t, b * 8], 1), :], (8, 128))
            for j in range(1, 8):
                r = jnp.broadcast_to(table[pl.ds(smem[t, b * 8 + j], 1), :], (8, 128))
                v = jnp.where(sub == j, r, v)
            parts.append(v)
        rows = jnp.concatenate(parts, axis=0).astype(bf16)
        total = total + lax.dot_general(rows, leafp[t], NT, preferred_element_type=f32)
    stress = lax.dot_general(tsp[...], total.astype(bf16), NT, preferred_element_type=f32)
    out_ref[...] = stress + near_acc[...]

    pltpu.make_async_copy(halobuf, halobuf, send_sem.at[2]).wait()
    pltpu.make_async_copy(closebuf, closebuf, send_sem.at[1]).wait()
    pltpu.make_async_copy(roots.at[0:N - 1], roots.at[0:N - 1], send_sem.at[3]).wait()
    pltpu.make_async_copy(sendbuf.at[0:COUNT], sendbuf.at[0:COUNT], send_sem.at[0]).wait()


def body(slip, to_multipole, up_shift, down_shift, sibling_far, leaf_far, to_stress, near_blocks,
         send_cells, far_list, near_list):
    up_shift, down_shift, sibling_far = (x.transpose(1, 0, 2) for x in (up_shift, down_shift, sibling_far))
    args = (slip, to_multipole, up_shift, down_shift, sibling_far, leaf_far, to_stress, near_blocks,
            send_cells.reshape(N, SLOTS), far_list, near_list)
    anywhere = pl.BlockSpec(memory_space=pl.ANY)
    return pl.pallas_call(
        step_kernel,
        out_shape=pltpu.VMEM((ELEM, CELLS), f32),
        in_specs=[anywhere] * len(args),
        out_specs=pl.BlockSpec(memory_space=pltpu.VMEM),
        scratch_shapes=[pltpu.VMEM(a.shape, a.dtype) for a in args] + [
            pltpu.VMEM((128, 128), bf16),
            pltpu.VMEM((128, 128), bf16),
            pltpu.VMEM((128, 128), f32),
            pltpu.VMEM((768, 128), bf16),
            pltpu.VMEM((384, 256), bf16),
            pltpu.VMEM((384, 256), bf16),
            pltpu.VMEM((KINDS, 128, 128), bf16),
            pltpu.VMEM((N, FAR, 128), bf16),
            pltpu.VMEM((8, SLOTS, 128), bf16),
            pltpu.VMEM((8, SLOTS, 128), bf16),
            pltpu.VMEM((2, HALO, ELEM), bf16),
            pltpu.VMEM((2, HALO, ELEM), bf16),
            pltpu.VMEM((N, FAR, 128), bf16),
            pltpu.VMEM((1, 128), f32),
            pltpu.VMEM((N, 1, 128), f32),
            pltpu.VMEM((256, 128), f32),
            pltpu.VMEM((256, 128), f32),
            pltpu.VMEM((256, 128), f32),
            pltpu.VMEM((256, 128), f32),
            pltpu.VMEM((256, 128), f32),
            pltpu.VMEM((ELEM, CELLS), f32),
            pltpu.VMEM((KINDS, CELLS), i32),
            pltpu.VMEM((ROWS, 128), f32),
            pltpu.SMEM((KINDS, CELLS), i32),
            pltpu.SemaphoreType.DMA((len(args),)),
            pltpu.SemaphoreType.DMA((4,)),
            pltpu.SemaphoreType.DMA((len(CUTS) - 1,)),
            pltpu.SemaphoreType.DMA,
            pltpu.SemaphoreType.DMA,
            pltpu.SemaphoreType.DMA,
            pltpu.SemaphoreType.DMA,
        ],
        compiler_params=pltpu.CompilerParams(collective_id=0, has_side_effects=True),
        name="step",
    )(*args)


def solution(mesh):
    cut = P(None, "leaf")
    return jax.shard_map(body, mesh=mesh,
                         in_specs=(cut, P(), P(), P(), P(), P(), P(), P(), P("leaf", None), cut, cut),
                         out_specs=cut, check_vma=False)
```

```python
import jax
import jax.numpy as jnp
from jax import lax
from jax.experimental import pallas as pl
from jax.experimental.pallas import tpu as pltpu
from jax.sharding import PartitionSpec as P

N = 128
CELLS = 256
COEF = 121
ELEM = 128
FAR = 32
SLOTS = 128
HALO = 32
KINDS = 27
NEAR = 9
CLOSE = (1, 2, 3, 4, 124, 125, 126, 127)
FIRST = 5
COUNT = 119


def hops(k):
    return sum(min(k // d % 4, 4 - k // d % 4) for d in (32, 8, 2))


ORDER = tuple(sorted((FIRST + i * 37 % COUNT for i in range(COUNT)), key=lambda k: -hops(k)))
ALL = tuple(sorted(range(1, N), key=lambda k: -hops(k)))
ROOTS_AFTER = 12
CUTS = (0, 30, 60, 90, 105, COUNT)
CLASS = {k: j for j in range(len(CUTS) - 1) for k in ORDER[CUTS[j]:CUTS[j + 1]]}
CLOSE_AFTER = 60
OWN_AT, CLOSE_AT, FAR_AT = 0, CELLS, CELLS + 8 * SLOTS
ROWS = FAR_AT + N * FAR
LEVEL_AT = (None, 0, 128, 192, 224, 240, 248, 252, 254)
BLOCK_AT = (0, 128, 192, 224, 240, 248, 252)
f32 = jnp.float32
bf16 = jnp.bfloat16
i32 = jnp.int32
MESH = pl.DeviceIdType.MESH
NT = (((1,), (1,)), ((), ()))
TN = (((0,), (0,)), ((), ()))


def mm(a, b):
    return jnp.dot(a, b, preferred_element_type=f32)


def split(x):
    high = x.astype(bf16)
    return high, (x - high.astype(f32)).astype(bf16)


def tripled(x):
    high, low = split(x)
    return jnp.concatenate([high, high, low], axis=1)


def onehot(index, count, axis, shape):
    return (index == lax.broadcasted_iota(i32, shape, axis)).astype(f32).astype(bf16)


def step_kernel(slip_hbm, wm_hbm, up_hbm, down_hbm, sib_hbm, leaf_hbm, ts_hbm, blocks_hbm, send_hbm, far_hbm, near_hbm,
                out_ref,
                slip, wm, up, down, sib, leaf, ts, blocks, send, far_list, near_list,
                wp, tsp, pad, up3, down3, sib3, leafp,
                sendbuf, closebuf, closein, halobuf, haloin, farin, rootbuf, roots,
                agg, blockagg, sibterm0, sibterm1, local, near_acc, indices, table, smem,
                load_sem, send_sem, far_sem, close_sem, halo_sem, root_sem, smem_sem):
    me = lax.axis_index("leaf")
    pairs = ((slip_hbm, slip), (wm_hbm, wm), (send_hbm, send), (up_hbm, up), (down_hbm, down), (sib_hbm, sib),
             (far_hbm, far_list), (near_hbm, near_list), (blocks_hbm, blocks), (ts_hbm, ts), (leaf_hbm, leaf))
    loads = [pltpu.make_async_copy(a, b, load_sem.at[i]) for i, (a, b) in enumerate(pairs)]
    for load in loads:
        load.start()
    barrier = pltpu.get_barrier_semaphore()

    for k in ALL:
        pl.semaphore_signal(barrier, inc=1, device_id=((me + k) & (N - 1),), device_id_type=MESH)

    wp[...] = jnp.zeros_like(wp)
    loads[0].wait()
    loads[1].wait()
    wp[0:COEF, :] = wm[...]
    mt = lax.dot_general(slip[...], wp[...], (((0,), (1,)), ((), ())), preferred_element_type=f32).astype(bf16)
    for side in range(2):
        pick = onehot(lax.broadcasted_iota(i32, (HALO, CELLS), 0) + (CELLS - HALO) * (1 - side), CELLS, 1, (HALO, CELLS))
        halobuf[side] = lax.dot_general(pick, slip[...], NT, preferred_element_type=f32).astype(bf16)

    loads[2].wait()
    lists = pltpu.roll(send[...].astype(f32).T, (N - me) & (N - 1), 1)
    lane = lax.broadcasted_iota(i32, (SLOTS, CELLS), 1).astype(f32)

    def peer(k):
        return ((me + k) & (N - 1),)

    def far_copy(k):
        return pltpu.make_async_remote_copy(
            src_ref=sendbuf.at[k], dst_ref=farin.at[k], send_sem=send_sem.at[0], recv_sem=far_sem.at[CLASS[k]],
            device_id=peer(k), device_id_type=MESH)

    def close_copy(i):
        return pltpu.make_async_remote_copy(
            src_ref=closebuf.at[i], dst_ref=closein.at[i], send_sem=send_sem.at[1], recv_sem=close_sem,
            device_id=peer(CLOSE[i]), device_id_type=MESH)

    def halo_copy(side):
        return pltpu.make_async_remote_copy(
            src_ref=halobuf.at[side], dst_ref=haloin.at[side], send_sem=send_sem.at[2], recv_sem=halo_sem,
            device_id=peer((1, N - 1)[side]), device_id_type=MESH)

    def root_copy(k):
        return pltpu.make_async_remote_copy(
            src_ref=rootbuf, dst_ref=roots.at[me], send_sem=send_sem.at[3], recv_sem=root_sem,
            device_id=peer(k), device_id_type=MESH)

    def fill(ks):
        for k in ks:
            hot = (lists[0:FAR, k:k + 1] == lane[0:FAR]).astype(f32).astype(bf16)
            sendbuf[k] = mm(hot, mt).astype(bf16)

    for i, k in enumerate(CLOSE):
        hot = (lists[:, k:k + 1] == lane).astype(f32).astype(bf16)
        closebuf[i] = mm(hot, mt).astype(bf16)
    fill(ORDER)

    pad[...] = jnp.zeros_like(pad)

    def padded_t(ref, s):
        pad[0:COEF, 0:COEF] = ref[:, s, :]
        return split(pad[...].T)

    loads[3].wait()
    for s in range(2):
        high, low = padded_t(up, s)
        up3[s * 128:s * 128 + 128, :] = high
        up3[256 + s * 128:256 + s * 128 + 128, :] = low
        up3[512 + s * 128:512 + s * 128 + 128, :] = high

    def pair_up(ref, at, count):
        pair = jnp.concatenate([ref[pl.ds(at, count, stride=2), :], ref[pl.ds(at + 1, count, stride=2), :]], axis=1)
        return mm(tripled(pair), up3[...])

    table[OWN_AT:OWN_AT + CELLS, :] = mt.astype(f32)
    agg[248:256, :] = jnp.zeros((8, 128), f32)
    agg[0:128, :] = pair_up(table, OWN_AT, 128)
    for level in range(1, 8):
        count = 128 >> level
        agg[pl.ds(LEVEL_AT[level + 1], count), :] = pair_up(agg, LEVEL_AT[level], count)
    root = agg[pl.ds(LEVEL_AT[8], 1), :]
    rootbuf[...] = root
    roots[me] = root

    pl.semaphore_wait(barrier, N - 1)

    for i in range(COUNT + 1):
        if i == 10:
            for side in range(2):
                halo_copy(side).start()
        if i % 12 == 11 and i // 12 < 8:
            close_copy(i // 12).start()
        if i == ROOTS_AFTER:
            for k in ALL:
                root_copy(k).start()
        if i < COUNT:
            far_copy(ORDER[i]).start()

    for load, ref, ref3 in ((loads[4], down, down3), (loads[5], sib, sib3)):
        load.wait()
        for s in range(2):
            high, low = padded_t(ref, s)
            ref3[0:128, s * 128:s * 128 + 128] = high
            ref3[128:256, s * 128:s * 128 + 128] = low
            ref3[256:384, s * 128:s * 128 + 128] = high
    sibs = mm(tripled(agg[...]), sib3[...])
    sibterm0[...] = sibs[:, 0:128]
    sibterm1[...] = sibs[:, 128:256]

    loads[6].wait()
    entry = far_list[...]
    rel = entry - CELLS
    sender = rel // SLOTS
    slot = rel - sender * SLOTS
    off = (me - sender) & (N - 1)
    close = jnp.where(off <= 4, off - 1, off - 120)
    is_close = (off <= 4) | (off >= 124)
    row = jnp.where(is_close, CLOSE_AT + close * SLOTS + slot, FAR_AT + off * FAR + slot)
    indices[...] = jnp.where(entry < CELLS, entry, row)
    to_smem = pltpu.make_async_copy(indices, smem, smem_sem)
    to_smem.start()

    loads[7].wait()
    loads[8].wait()
    loads[9].wait()
    pltpu.make_async_copy(halobuf, haloin, halo_sem).wait()
    left = jnp.where(me > 0, haloin[0].astype(f32), 0.0)
    right = jnp.where(me < N - 1, haloin[1].astype(f32), 0.0)
    edge = jnp.concatenate([left, right], axis=0).T.astype(bf16)
    own = slip[...]
    near_acc[...] = jnp.zeros_like(near_acc)
    for k in range(NEAR):
        w = near_list[k:k + 1, :]
        at = jnp.where(w < HALO, w + CELLS, jnp.where(w < HALO + CELLS, w - HALO, w))
        hot = onehot(at, 0, 0, (CELLS + 2 * HALO, CELLS))
        cols = mm(own, hot[0:CELLS]) + mm(edge, hot[CELLS:])
        near_acc[...] += mm(blocks[k], cols.astype(bf16))
    tsp[...] = jnp.zeros_like(tsp)
    tsp[:, 0:COEF] = ts[...]

    pltpu.make_async_copy(roots.at[0:N - 1], roots.at[0:N - 1], root_sem).wait()
    blockagg[0:N, :] = roots[...].reshape(N, 128)
    for bit in range(6):
        count = 64 >> bit
        blockagg[pl.ds(BLOCK_AT[bit + 1], count), :] = pair_up(blockagg, BLOCK_AT[bit], count)
    branch = [(me >> bit) & 1 for bit in range(7)]
    rows = [blockagg[pl.ds(BLOCK_AT[bit] + ((me >> bit) ^ 1), 1), :] for bit in range(7)]
    terms = mm(tripled(jnp.concatenate(rows + [rows[0]], axis=0)), sib3[...])
    expansion = jnp.zeros((8, 128), f32)
    for bit in reversed(range(7)):
        both = jnp.broadcast_to(terms[bit:bit + 1, :], (8, 256))
        if bit < 6:
            both = both + mm(tripled(expansion), down3[...])
        expansion = jnp.where(branch[bit] == 0, both[:, 0:128], both[:, 128:256])

    local[0:8, :] = jnp.zeros((8, 128), f32)
    for level in reversed(range(8)):
        count = 128 >> level
        both = mm(tripled(expansion), down3[...])
        low, high = both[0:count, 0:128], both[0:count, 128:256]
        if level >= 1:
            at = LEVEL_AT[level]
            low = low + sibterm0[pl.ds(at + 1, count, stride=2), :]
            high = high + sibterm1[pl.ds(at, count, stride=2), :]
        local[pl.ds(0, count, stride=2), :] = low
        local[pl.ds(1, count, stride=2), :] = high
        expansion = local[0:max(2 * count, 8), :]

    leafp[...] = jnp.zeros_like(leafp)
    loads[10].wait()
    for t in range(KINDS):
        leafp[t, 0:COEF, 0:COEF] = leaf[t]

    pltpu.make_async_copy(closebuf, closein, close_sem).wait()
    for i in range(8):
        table[CLOSE_AT + i * SLOTS:CLOSE_AT + (i + 1) * SLOTS, :] = closein[i].astype(f32)
    to_smem.wait()
    for j in range(len(CUTS) - 1):
        count = CUTS[j + 1] - CUTS[j]
        pltpu.make_async_copy(farin.at[0:count], farin.at[0:count], far_sem.at[j]).wait()
        for k in ORDER[CUTS[j]:CUTS[j + 1]]:
            table[FAR_AT + k * FAR:FAR_AT + (k + 1) * FAR, :] = farin[k].astype(f32)

    sub = lax.broadcasted_iota(i32, (8, 128), 0)
    total = local[...]
    for t in range(KINDS):
        parts = []
        for b in range(CELLS // 8):
            v = jnp.broadcast_to(table[pl.ds(smem[t, b * 8], 1), :], (8, 128))
            for j in range(1, 8):
                r = jnp.broadcast_to(table[pl.ds(smem[t, b * 8 + j], 1), :], (8, 128))
                v = jnp.where(sub == j, r, v)
            parts.append(v)
        rows = jnp.concatenate(parts, axis=0).astype(bf16)
        total = total + lax.dot_general(rows, leafp[t], NT, preferred_element_type=f32)
    stress = lax.dot_general(tsp[...], total.astype(bf16), NT, preferred_element_type=f32)
    out_ref[...] = stress + near_acc[...]

    pltpu.make_async_copy(halobuf, halobuf, send_sem.at[2]).wait()
    pltpu.make_async_copy(closebuf, closebuf, send_sem.at[1]).wait()
    pltpu.make_async_copy(roots.at[0:N - 1], roots.at[0:N - 1], send_sem.at[3]).wait()
    pltpu.make_async_copy(sendbuf.at[0:COUNT], sendbuf.at[0:COUNT], send_sem.at[0]).wait()


def body(slip, to_multipole, up_shift, down_shift, sibling_far, leaf_far, to_stress, near_blocks,
         send_cells, far_list, near_list):
    up_shift, down_shift, sibling_far = (x.transpose(1, 0, 2) for x in (up_shift, down_shift, sibling_far))
    args = (slip, to_multipole, up_shift, down_shift, sibling_far, leaf_far, to_stress, near_blocks,
            send_cells.reshape(N, SLOTS), far_list, near_list)
    anywhere = pl.BlockSpec(memory_space=pl.ANY)
    return pl.pallas_call(
        step_kernel,
        out_shape=pltpu.VMEM((ELEM, CELLS), f32),
        in_specs=[anywhere] * len(args),
        out_specs=pl.BlockSpec(memory_space=pltpu.VMEM),
        scratch_shapes=[pltpu.VMEM(a.shape, a.dtype) for a in args] + [
            pltpu.VMEM((128, 128), bf16),
            pltpu.VMEM((128, 128), bf16),
            pltpu.VMEM((128, 128), f32),
            pltpu.VMEM((768, 128), bf16),
            pltpu.VMEM((384, 256), bf16),
            pltpu.VMEM((384, 256), bf16),
            pltpu.VMEM((KINDS, 128, 128), bf16),
            pltpu.VMEM((N, FAR, 128), bf16),
            pltpu.VMEM((8, SLOTS, 128), bf16),
            pltpu.VMEM((8, SLOTS, 128), bf16),
            pltpu.VMEM((2, HALO, ELEM), bf16),
            pltpu.VMEM((2, HALO, ELEM), bf16),
            pltpu.VMEM((N, FAR, 128), bf16),
            pltpu.VMEM((1, 128), f32),
            pltpu.VMEM((N, 1, 128), f32),
            pltpu.VMEM((256, 128), f32),
            pltpu.VMEM((256, 128), f32),
            pltpu.VMEM((256, 128), f32),
            pltpu.VMEM((256, 128), f32),
            pltpu.VMEM((256, 128), f32),
            pltpu.VMEM((ELEM, CELLS), f32),
            pltpu.VMEM((KINDS, CELLS), i32),
            pltpu.VMEM((ROWS, 128), f32),
            pltpu.SMEM((KINDS, CELLS), i32),
            pltpu.SemaphoreType.DMA((len(args),)),
            pltpu.SemaphoreType.DMA((4,)),
            pltpu.SemaphoreType.DMA((len(CUTS) - 1,)),
            pltpu.SemaphoreType.DMA,
            pltpu.SemaphoreType.DMA,
            pltpu.SemaphoreType.DMA,
            pltpu.SemaphoreType.DMA,
        ],
        compiler_params=pltpu.CompilerParams(collective_id=0, has_side_effects=True),
        name="step",
    )(*args)


def solution(mesh):
    cut = P(None, "leaf")
    return jax.shard_map(body, mesh=mesh,
                         in_specs=(cut, P(), P(), P(), P(), P(), P(), P(), P("leaf", None), cut, cut),
                         out_specs=cut, check_vma=False)
```
